32 devices in a mesh: case: 4 (over z), gx: 2 (over y), gy: 4 (over x, core).
Axes of the slice: x: 2, y: 2, z: 4, core: 2. Of those that a mesh axis runs over, the one named last changes fastest.
Arguments:
- load: float32 [8, 24, 32, 128], P(('case', 'gx'), 'gy'), parts along dimension 0, may hold values from -4 to 4
- factors: bfloat16 [4, 8, 24, 128, 128], P(None, ('case', 'gx'), 'gy'), parts along dimension 1, may hold values from -6 to 6
- links: int32 [4, 8, 24], P(None, ('case', 'gx'), 'gy'), parts along dimension 1, may hold values from 0 to 1
- shift: float32 [8, 24, 128], P(('case', 'gx'), 'gy'), parts along dimension 0, may hold values from 0.25 to 2.5
Outputs:
- solution: float32 [8, 24, 32, 128], P(('case', 'gx'), 'gy'), parts along dimension 0
- residual: float32 [8, 24, 32, 128], P(('case', 'gx'), 'gy'), parts along dimension 0
The draws below stay inside these ranges and needn't reach their ends.
There are 4 independent parts, one for each index of `case`. The reference program is written for one: setup_inputs(seed, part) draws one part's arguments, and reference() takes and returns one part's arrays. A program takes and returns all parts, laid end to end along the dimension named above; each array names one. Nothing has to cross between parts.
All inputs are finite; a program needn't handle non-finite values.
Results may differ from the reference program's by a relative error of at most 0.008.
Values may be sent and summed in bfloat16 or wider, within the bound.
No kernel may reach another device: no remote copies, remote signals or barrier semaphores. Data moves between devices by JAX's collectives and lax.ppermute only.
A program may use at most 64 MiB of HBM per device.

```python
import jax
import jax.numpy as jnp
from jax import lax

B = 128
NBX = 1
NBY = 6
NRHS = 32
ITERS = 8
NX = 2
NY = 24


OFFSETS = ((1, 0), (0, 1), (1, 1), (1, -1))


def displaced(array, step_x, step_y):
    padded = jnp.pad(array, ((1, 1), (1, 1)))
    return padded[1 + step_x:1 + step_x + NX, 1 + step_y:1 + step_y + NY]


def spike_plan(key):
    spike_key = jax.random.fold_in(key, 501)
    shards_x = NX // NBX
    shards_y = NY // NBY
    row_pick = jax.random.randint(jax.random.fold_in(spike_key, 1), (shards_x, shards_y), 0, NBX)
    column_pick = jax.random.randint(jax.random.fold_in(spike_key, 2), (shards_x, shards_y), 0, NBY - 1)
    active = jax.random.randint(jax.random.fold_in(spike_key, 3), (shards_x, shards_y), 0, 4)

    def expand(values):
        return jnp.repeat(jnp.repeat(values, NBX, axis=0), NBY, axis=1)
    local_x = jnp.arange(NX, dtype=jnp.int32) % NBX
    local_y = jnp.arange(NY, dtype=jnp.int32) % NBY
    chosen = (expand(active) > 0) & (local_x[:, None] == expand(row_pick)) & (local_y[None, :] == expand(column_pick))
    anchor = chosen.astype(jnp.int32)
    partner = displaced(anchor, 0, -1)
    marked = jnp.maximum(anchor, partner)
    return (anchor, marked)


def draw_load(key, part):
    sample = jax.random.normal(jax.random.fold_in(key, 11), (NX, NY, NRHS, B), jnp.float32)
    sample = jnp.clip(sample, -4.0, 4.0)
    return sample


def draw_links(key, part):
    anchor, marked = spike_plan(key)
    coupled = (jax.random.randint(jax.random.fold_in(key, 23), (4, NX, NY), 0, 4) > 0).astype(jnp.int32)
    touches = jnp.stack([jnp.maximum(marked, displaced(marked, step_x, step_y)) for step_x, step_y in OFFSETS])
    kept = coupled * (1 - touches)
    empty = jnp.zeros((NX, NY), jnp.int32)
    spiked = jnp.stack([empty, anchor, empty, empty])
    return jnp.maximum(kept, spiked).astype(jnp.int32)


def draw_factors(key, part):
    anchor, marked = spike_plan(key)
    noise = jax.random.normal(jax.random.fold_in(key, 37), (4, NX, NY, B, B), jnp.float32)
    noise = jnp.clip(noise, -6.0, 6.0)
    left = jax.random.randint(jax.random.fold_in(key, 43), (NX, NY, B), 0, 2).astype(jnp.float32) * 2.0 - 1.0
    right = jax.random.randint(jax.random.fold_in(key, 47), (NX, NY, B), 0, 2).astype(jnp.float32) * 2.0 - 1.0
    weight = 4.0 * anchor.astype(jnp.float32)[:, :, None, None]
    spike = weight * left[:, :, :, None] * right[:, :, None, :]
    noise = noise.at[1].add(spike)
    return jnp.clip(noise, -6.0, 6.0).astype(jnp.bfloat16)


def draw_shift(key, part):
    anchor, marked = spike_plan(key)
    values = jax.random.uniform(jax.random.fold_in(key, 41), (NX, NY, B), jnp.float32, 0.25, 2.5)
    return jnp.where(marked[:, :, None] > 0, 0.5, values).astype(jnp.float32)


def setup_inputs(seed: int = 0, part: int = 0) -> dict:
    arg_keys = jax.random.split(jax.random.key(seed), 5)
    own_keys = jax.random.split(jax.random.fold_in(arg_keys[4], part), 5)
    return {
        "load": draw_load(jax.random.fold_in(jax.random.fold_in(arg_keys[4], part), 71), part),
        "factors": draw_factors(jax.random.fold_in(jax.random.fold_in(arg_keys[4], part), 71), part),
        "links": draw_links(jax.random.fold_in(jax.random.fold_in(arg_keys[4], part), 71), part),
        "shift": draw_shift(jax.random.fold_in(jax.random.fold_in(arg_keys[4], part), 71), part),
    }


OFFSETS = ((1, 0), (0, 1), (1, 1), (1, -1))
PRECISE = lax.Precision.HIGHEST

def neighbour(array, step_x, step_y):
    count_x, count_y = (array.shape[0], array.shape[1])
    widths = ((1, 1), (1, 1)) + ((0, 0),) * (array.ndim - 2)
    padded = jnp.pad(array, widths)
    return padded[1 + step_x:1 + step_x + count_x, 1 + step_y:1 + step_y + count_y]

def apply_block(block, field):
    return jnp.einsum('xyab,xyrb->xyra', block.astype(jnp.float32), field.astype(jnp.float32), precision=PRECISE, preferred_element_type=jnp.float32)

def inner(left, right):
    return jnp.sum(left * right, axis=(0, 1, 3))

def spread(values):
    return values[None, None, :, None]

def reference(load, factors, links, shift):
    masked = factors.astype(jnp.float32) * links.astype(jnp.float32)[:, :, :, None, None]
    springs = jnp.einsum('dxyak,dxybk->dxyab', masked.astype(jnp.float32), masked.astype(jnp.float32), precision=PRECISE, preferred_element_type=jnp.float32) / B
    forward = [springs[offset] for offset in range(4)]
    backward = [neighbour(springs[offset], -OFFSETS[offset][0], -OFFSETS[offset][1]) for offset in range(4)]
    identity = jnp.eye(B, dtype=jnp.float32)
    diagonal = shift[..., None] * identity + sum(forward) + sum(backward)
    flat = diagonal.reshape(-1, B, B)
    lower = jnp.linalg.cholesky(flat)
    inverse = jax.vmap(lambda factor: jax.scipy.linalg.cho_solve((factor, True), identity))(lower).reshape(diagonal.shape)

    def operate(field):
        result = apply_block(diagonal, field)
        for offset in range(4):
            step_x, step_y = OFFSETS[offset]
            result = result - apply_block(forward[offset], neighbour(field, step_x, step_y))
            result = result - apply_block(backward[offset], neighbour(field, -step_x, -step_y))
        return result
    solution = jnp.zeros_like(load)
    residual = load
    precon = apply_block(inverse, residual)
    direction = precon
    rz_now = inner(residual, precon)
    for iteration in range(ITERS):
        image = operate(direction)
        alpha = rz_now / inner(direction, image)
        solution = solution + spread(alpha) * direction
        residual = residual - spread(alpha) * image
        precon = apply_block(inverse, residual)
        rz_next = inner(residual, precon)
        direction = precon + spread(rz_next / rz_now) * direction
        rz_now = rz_next
    return (solution, residual)
```

```python
import jax
import jax.numpy as jnp
from jax import lax
from jax.experimental import pallas as pl
from jax.experimental.pallas import tpu as pltpu
from jax.sharding import PartitionSpec as P

B = 128
ITERS = 8


OFFSETS = ((1, 0), (0, 1), (1, 1), (1, -1))
PRECISE = lax.Precision.HIGHEST


def extended(cells, sides, width):
    for axis, dim in sides:
        count = lax.axis_size(axis)
        ends = count - 1
        head = lax.slice_in_dim(cells, 0, width, axis=dim)
        tail = lax.slice_in_dim(cells, cells.shape[dim] - width, cells.shape[dim], axis=dim)
        cells = jnp.concatenate(
            [
                lax.ppermute(tail, axis, [(i, (i + 1) % count) for i in range(ends)]),
                cells,
                lax.ppermute(head, axis, [((i + 1) % count, i) for i in range(ends)]),
            ],
            axis=dim,
        )
    return cells


def window(padded, step_x, step_y, count_x, count_y):
    return padded[1 + step_x : 1 + step_x + count_x, 1 + step_y : 1 + step_y + count_y]


def inner(left, right):
    return jnp.sum(left * right, axis=(0, 1, 3))


def spread(values):
    return values[None, None, :, None]


def local_halo(load, factors, links, shift):
    count_x, count_y = (load.shape[0], load.shape[1])
    masked = factors * links.astype(jnp.bfloat16)[:, :, :, None, None]
    springs = (
        jnp.einsum("dxyak,dxybk->dxyab", masked, masked, preferred_element_type=jnp.float32) / B
    )
    padded_springs = extended(springs, (("gx", 1), ("gy", 2)), 1)
    forward = padded_springs[:, 1:-1, 1:-1]
    backward = jnp.stack(
        [
            window(
                padded_springs[offset], -OFFSETS[offset][0], -OFFSETS[offset][1], count_x, count_y
            )
            for offset in range(4)
        ]
    )
    identity = jnp.eye(B, dtype=jnp.float32)
    diagonal = shift[..., None] * identity + jnp.sum(forward, axis=0) + jnp.sum(backward, axis=0)
    lower = jnp.linalg.cholesky(diagonal.reshape(-1, B, B))
    inverse = jax.vmap(lambda factor: jax.scipy.linalg.cho_solve((factor, True), identity))(
        lower
    ).reshape(diagonal.shape)
    blocks = jnp.concatenate([diagonal[None], -forward, -backward], axis=0)

    def operate(field):
        padded = extended(field, (("gx", 0), ("gy", 1)), 1)
        pieces = [field]
        pieces = pieces + [
            window(padded, step_x, step_y, count_x, count_y) for step_x, step_y in OFFSETS
        ]
        pieces = pieces + [
            window(padded, -step_x, -step_y, count_x, count_y) for step_x, step_y in OFFSETS
        ]
        return jnp.einsum(
            "kxyab,kxyrb->xyra",
            blocks,
            jnp.stack(pieces),
            precision=PRECISE,
            preferred_element_type=jnp.float32,
        )

    def precondition(field):
        return jnp.einsum(
            "xyab,xyrb->xyra", inverse, field, precision=PRECISE, preferred_element_type=jnp.float32
        )

    def paired(residual, precon, image):
        return lax.psum((inner(residual, precon), inner(image, precon)), ("gx", "gy"))

    solution = jnp.zeros_like(load)
    residual = load
    precon = precondition(residual)
    image = operate(precon)
    gamma, delta = paired(residual, precon, image)
    alpha = gamma / delta
    direction, along = (precon, image)
    for iteration in range(ITERS):
        solution = solution + spread(alpha) * direction
        residual = residual - spread(alpha) * along
        if iteration + 1 < ITERS:
            precon = precondition(residual)
            image = operate(precon)
            gamma_next, delta = paired(residual, precon, image)
            ratio = gamma_next / gamma
            alpha = gamma_next / (delta - ratio * gamma_next / alpha)
            direction = precon + spread(ratio) * direction
            along = image + spread(ratio) * along
            gamma = gamma_next
    return (solution, residual)


GRID_AXES = ("gx", "gy")
ROWS = 4
VMEM = pl.BlockSpec(memory_space=pltpu.VMEM)
VMEM_BYTES = 56 * 1024 * 1024


def gram(block):
    return (
        lax.dot_general(block, block, (((1,), (1,)), ((), ())), preferred_element_type=jnp.float32)
        / B
    )


def split(value):
    first = value.astype(jnp.bfloat16)
    rest = value - first.astype(jnp.float32)
    second = rest.astype(jnp.bfloat16)
    third = (rest - second.astype(jnp.float32)).astype(jnp.bfloat16)
    return first, second, third


def invert_kernel(ahead, behind, shift, out, work):
    nodes = shift.shape[0]
    rows = lax.broadcasted_iota(jnp.int32, (B, B), 0)
    lanes = lax.broadcasted_iota(jnp.int32, (B, B), 1)
    for node in range(nodes):
        total = jnp.where(rows == lanes, shift[pl.ds(node, 1), :], 0.0)
        for d in range(len(OFFSETS)):
            total = total + gram(ahead[d, node])
            total = total + gram(behind[d, node])
        work[node] = total

    def step(k, carry):
        lane = lax.broadcasted_iota(jnp.int32, (1, B), 1)
        for node in range(nodes):
            block = work[node]
            row = work[node, pl.ds(k, 1), :]
            column = jnp.take_along_axis(block, jnp.full((B, B), k, jnp.int32), axis=1)
            pivot = jnp.sum(jnp.where(lane == k, row, 0.0), axis=1, keepdims=True)
            scaled = jnp.where(lane == k, 1.0, row) / pivot
            work[node] = jnp.where(lanes == k, 0.0, block) - column * scaled
            work[node, pl.ds(k, 1), :] = scaled
        return carry

    lax.fori_loop(0, B, step, 0)
    for node in range(nodes):
        out[node] = work[node]


def invert(ahead, behind, shift):
    nodes = shift.shape[0]
    return pl.pallas_call(
        invert_kernel,
        out_shape=jax.ShapeDtypeStruct((nodes, B, B), jnp.float32),
        in_specs=[VMEM] * 3,
        out_specs=VMEM,
        scratch_shapes=[pltpu.VMEM((nodes, B, B), jnp.float32)],
    )(ahead, behind, shift)


def stacked(value):
    first, second, third = (term.astype(jnp.float32) for term in split(value))
    upper = lax.broadcasted_iota(jnp.int32, value.shape, 0) < ROWS
    both = [jnp.where(upper, first, second), jnp.where(upper, third, 0.0)]
    return jnp.concatenate(both, axis=0).astype(jnp.bfloat16)


def product(left, right):
    full = jnp.dot(left, right, preferred_element_type=jnp.float32)
    total = full[: 2 * ROWS, :B] + full[2 * ROWS :, :B]
    for part in range(1, right.shape[1] // B):
        total = total + full[: 2 * ROWS, part * B : (part + 1) * B]
    return total + jnp.concatenate([total[ROWS:], total[:ROWS]], axis=0)


def solve_kernel(nx, ny, nbx, nby):
    ncy = ny // nby
    devices = (nx // nbx) * ncy
    unroll = 2 if ny % 2 == 0 else 1

    def kernel(load, shift, factors, inverse, out_x, out_r, w, m, p, q, image, x, r, z, mass):
        def prepare(dev, carry):
            for lx in range(nbx):
                for ly in range(nby):
                    gx, gy = (dev // ncy) * nbx + lx, (dev % ncy) * nby + ly
                    node = lx * nby + ly
                    for d in range(len(OFFSETS)):
                        first, second, _ = split(gram(factors[dev, d, node]))
                        w[d, gx, gy, :, :B] = first
                        w[d, gx, gy, :, B:] = second
                    for part, term in enumerate(split(inverse[dev, node])):
                        m[gx, gy, :, part * B : (part + 1) * B] = term
                    field = load[dev, node]
                    r[gx, gy] = jnp.concatenate([field, field], axis=0)
                    mass[gx, gy] = jnp.broadcast_to(shift[dev, pl.ds(node, 1), :], (2 * ROWS, B))
            return carry

        lax.fori_loop(0, devices, prepare, 0)
        p[...] = jnp.zeros_like(p)
        q[...] = jnp.zeros_like(q)
        x[...] = jnp.zeros_like(x)
        zero = jnp.zeros((2 * ROWS, B), jnp.float32)

        def total(values):
            return jnp.sum(values, axis=1, keepdims=True)

        def iterate(_, rz_old):
            def precondition(y, acc):
                for i in range(nx):
                    value = r[i, y]
                    precon = product(stacked(value), m[i, y])
                    z[i, y] = precon
                    acc = acc + value * precon
                return acc

            rz = total(lax.fori_loop(0, ny, precondition, zero, unroll=2 * unroll))
            ratio = rz / rz_old

            def advance(y, carry):
                for i in range(nx):
                    p[1 + i, 1 + y] = z[i, y] + ratio * p[1 + i, 1 + y]
                return carry

            lax.fori_loop(0, ny, advance, 0, unroll=2 * unroll)

            def edges(y, carry):
                for i in range(nx):
                    for d, (step_x, step_y) in enumerate(OFFSETS):
                        delta = p[1 + i, 1 + y] - p[1 + i + step_x, 1 + y + step_y]
                        q[d, 1 + i, 1 + y] = product(stacked(delta), w[d, i, y])
                return carry

            lax.fori_loop(0, ny, edges, 0, unroll=unroll)

            def gather(y, acc):
                for i in range(nx):
                    value = p[1 + i, 1 + y]
                    result = mass[i, y] * value
                    for d, (step_x, step_y) in enumerate(OFFSETS):
                        result = result + (
                            q[d, 1 + i, 1 + y] - q[d, 1 + i - step_x, 1 + y - step_y]
                        )
                    image[i, y] = result
                    acc = acc + value * result
                return acc

            alpha = rz / total(lax.fori_loop(0, ny, gather, zero, unroll=2 * unroll))

            def update(y, carry):
                for i in range(nx):
                    x[i, y] = x[i, y] + alpha * p[1 + i, 1 + y]
                    r[i, y] = r[i, y] - alpha * image[i, y]
                return carry

            lax.fori_loop(0, ny, update, 0, unroll=2 * unroll)
            return rz

        lax.fori_loop(0, ITERS, iterate, jnp.ones((2 * ROWS, 1), jnp.float32))

        def finish(dev, carry):
            for lx in range(nbx):
                for ly in range(nby):
                    gx, gy = (dev // ncy) * nbx + lx, (dev % ncy) * nby + ly
                    out_x[dev, lx * nby + ly] = x[gx, gy][:ROWS]
                    out_r[dev, lx * nby + ly] = r[gx, gy][:ROWS]
            return carry

        lax.fori_loop(0, devices, finish, 0)

    return kernel


def solve(load, shift, factors, inverse, nx, ny, nbx, nby):
    tall = 2 * ROWS
    field = pltpu.VMEM((nx, ny, tall, B), jnp.float32)
    return pl.pallas_call(
        solve_kernel(nx, ny, nbx, nby),
        out_shape=[jax.ShapeDtypeStruct(load.shape, jnp.float32)] * 2,
        in_specs=[VMEM] * 4,
        out_specs=[VMEM] * 2,
        scratch_shapes=[
            pltpu.VMEM((len(OFFSETS), nx, ny, B, 2 * B), jnp.bfloat16),
            pltpu.VMEM((nx, ny, B, 3 * B), jnp.bfloat16),
            pltpu.VMEM((nx + 2, ny + 2, tall, B), jnp.float32),
            pltpu.VMEM((len(OFFSETS), nx + 2, ny + 2, tall, B), jnp.float32),
        ]
        + [field] * 5,
        compiler_params=pltpu.CompilerParams(vmem_limit_bytes=VMEM_BYTES),
    )(load, shift, factors, inverse)


def shifted(cells, axis, dim, step):
    count = lax.axis_size(axis)
    size = cells.shape[dim]
    if step == 1:
        rim = lax.slice_in_dim(cells, size - 1, size, axis=dim)
        rim = lax.ppermute(rim, axis, [(i, i + 1) for i in range(count - 1)])
        return jnp.concatenate([rim, lax.slice_in_dim(cells, 0, size - 1, axis=dim)], axis=dim)
    rim = lax.slice_in_dim(cells, 0, 1, axis=dim)
    rim = lax.ppermute(rim, axis, [(i + 1, i) for i in range(count - 1)])
    return jnp.concatenate([lax.slice_in_dim(cells, 1, size, axis=dim), rim], axis=dim)


def local_columns(load, factors, links, shift):
    nbx, nby, rhs, _ = load.shape
    gx, gy = (lax.axis_size(axis) for axis in GRID_AXES)
    devices, nodes = gx * gy, nbx * nby
    masked = factors * links.astype(jnp.bfloat16)[:, :, :, None, None]
    gathered = lax.all_gather(masked.reshape(4, nodes, B, B), GRID_AXES)
    down = shifted(jnp.stack([masked[0], masked[2], masked[3]]), "gx", 1, 1)
    left = shifted(jnp.stack([masked[1], down[1]]), "gy", 2, 1)
    right = shifted(down[2:], "gy", 2, -1)
    behind = jnp.stack([down[0], left[0], left[1], right[0]])
    flat_shift = shift.reshape(nodes, B)
    inverse = invert(
        masked.reshape(4, nodes, B, B), behind.reshape(4, nodes, B, B), flat_shift
    )
    columns = load.reshape(nodes, devices, ROWS, B).transpose(1, 0, 2, 3)
    columns = lax.all_to_all(columns, GRID_AXES, 0, 0)
    shifts = lax.all_gather(flat_shift, GRID_AXES)
    inverses = lax.all_gather(inverse, GRID_AXES)
    outs = solve(columns, shifts, gathered, inverses, gx * nbx, gy * nby, nbx, nby)
    outs = lax.all_to_all(jnp.stack(outs, axis=1), GRID_AXES, 0, 0)
    outs = outs.transpose(1, 2, 0, 3, 4).reshape(2, nbx, nby, rhs, B)
    return (outs[0], outs[1])


def local(load, factors, links, shift):
    devices = lax.axis_size("gx") * lax.axis_size("gy")
    blocks = devices * load.shape[0] * load.shape[1]
    held = blocks * B * B * (len(OFFSETS) * 6 + 10)
    if load.shape[2] == ROWS * devices and held < VMEM_BYTES * 3 // 4:
        return local_columns(load, factors, links, shift)
    return local_halo(load, factors, links, shift)


def solution(mesh):
    placed = (
        P(("case", "gx"), "gy", None, None),
        P(None, ("case", "gx"), "gy", None, None),
        P(None, ("case", "gx"), "gy"),
        P(("case", "gx"), "gy", None),
    )
    return jax.shard_map(
        local,
        mesh=mesh,
        in_specs=placed,
        out_specs=(P(("case", "gx"), "gy", None, None), P(("case", "gx"), "gy", None, None)),
        check_vma=False,
    )
```

```python
import jax
import jax.numpy as jnp
from jax import lax
from jax.experimental import pallas as pl
from jax.experimental.pallas import tpu as pltpu
from jax.sharding import PartitionSpec as P

B = 128
ITERS = 8


OFFSETS = ((1, 0), (0, 1), (1, 1), (1, -1))
PRECISE = lax.Precision.HIGHEST


def extended(cells, sides, width):
    for axis, dim in sides:
        count = lax.axis_size(axis)
        ends = count - 1
        head = lax.slice_in_dim(cells, 0, width, axis=dim)
        tail = lax.slice_in_dim(cells, cells.shape[dim] - width, cells.shape[dim], axis=dim)
        cells = jnp.concatenate(
            [
                lax.ppermute(tail, axis, [(i, (i + 1) % count) for i in range(ends)]),
                cells,
                lax.ppermute(head, axis, [((i + 1) % count, i) for i in range(ends)]),
            ],
            axis=dim,
        )
    return cells


def window(padded, step_x, step_y, count_x, count_y):
    return padded[1 + step_x : 1 + step_x + count_x, 1 + step_y : 1 + step_y + count_y]


def inner(left, right):
    return jnp.sum(left * right, axis=(0, 1, 3))


def spread(values):
    return values[None, None, :, None]


def local_halo(load, factors, links, shift):
    count_x, count_y = (load.shape[0], load.shape[1])
    masked = factors * links.astype(jnp.bfloat16)[:, :, :, None, None]
    springs = (
        jnp.einsum("dxyak,dxybk->dxyab", masked, masked, preferred_element_type=jnp.float32) / B
    )
    padded_springs = extended(springs, (("gx", 1), ("gy", 2)), 1)
    forward = padded_springs[:, 1:-1, 1:-1]
    backward = jnp.stack(
        [
            window(
                padded_springs[offset], -OFFSETS[offset][0], -OFFSETS[offset][1], count_x, count_y
            )
            for offset in range(4)
        ]
    )
    identity = jnp.eye(B, dtype=jnp.float32)
    diagonal = shift[..., None] * identity + jnp.sum(forward, axis=0) + jnp.sum(backward, axis=0)
    lower = jnp.linalg.cholesky(diagonal.reshape(-1, B, B))
    inverse = jax.vmap(lambda factor: jax.scipy.linalg.cho_solve((factor, True), identity))(
        lower
    ).reshape(diagonal.shape)
    blocks = jnp.concatenate([diagonal[None], -forward, -backward], axis=0)

    def operate(field):
        padded = extended(field, (("gx", 0), ("gy", 1)), 1)
        pieces = [field]
        pieces = pieces + [
            window(padded, step_x, step_y, count_x, count_y) for step_x, step_y in OFFSETS
        ]
        pieces = pieces + [
            window(padded, -step_x, -step_y, count_x, count_y) for step_x, step_y in OFFSETS
        ]
        return jnp.einsum(
            "kxyab,kxyrb->xyra",
            blocks,
            jnp.stack(pieces),
            precision=PRECISE,
            preferred_element_type=jnp.float32,
        )

    def precondition(field):
        return jnp.einsum(
            "xyab,xyrb->xyra", inverse, field, precision=PRECISE, preferred_element_type=jnp.float32
        )

    def paired(residual, precon, image):
        return lax.psum((inner(residual, precon), inner(image, precon)), ("gx", "gy"))

    solution = jnp.zeros_like(load)
    residual = load
    precon = precondition(residual)
    image = operate(precon)
    gamma, delta = paired(residual, precon, image)
    alpha = gamma / delta
    direction, along = (precon, image)
    for iteration in range(ITERS):
        solution = solution + spread(alpha) * direction
        residual = residual - spread(alpha) * along
        if iteration + 1 < ITERS:
            precon = precondition(residual)
            image = operate(precon)
            gamma_next, delta = paired(residual, precon, image)
            ratio = gamma_next / gamma
            alpha = gamma_next / (delta - ratio * gamma_next / alpha)
            direction = precon + spread(ratio) * direction
            along = image + spread(ratio) * along
            gamma = gamma_next
    return (solution, residual)


GRID_AXES = ("gx", "gy")
ROWS = 4
VMEM = pl.BlockSpec(memory_space=pltpu.VMEM)
VMEM_BYTES = 56 * 1024 * 1024


def gram(block):
    return (
        lax.dot_general(block, block, (((1,), (1,)), ((), ())), preferred_element_type=jnp.float32)
        / B
    )


def split(value):
    first = value.astype(jnp.bfloat16)
    rest = value - first.astype(jnp.float32)
    second = rest.astype(jnp.bfloat16)
    third = (rest - second.astype(jnp.float32)).astype(jnp.bfloat16)
    return first, second, third


def invert_kernel(ahead, behind, shift, out, *work):
    nodes = shift.shape[0]
    rows = lax.broadcasted_iota(jnp.int32, (B, B), 0)
    lanes = lax.broadcasted_iota(jnp.int32, (B, B), 1)
    for node in range(nodes):
        total = jnp.where(rows == lanes, shift[pl.ds(node, 1), :], 0.0)
        for d in range(len(OFFSETS)):
            total = total + gram(ahead[d, node])
            total = total + gram(behind[d, node])
        work[node][...] = total

    def step(k, carry):
        lane = lax.broadcasted_iota(jnp.int32, (nodes, B), 1)
        picked = jnp.concatenate([block[pl.ds(k, 1), :] for block in work], axis=0)
        pivot = jnp.sum(jnp.where(lane == k, picked, 0.0), axis=1, keepdims=True)
        scaled = jnp.where(lane == k, 1.0, picked) / pivot
        index = jnp.full((8, B), k, jnp.int32)
        other = lane[:1] == k
        for node, block in enumerate(work):
            row = scaled[node : node + 1]
            for top in range(0, B, 8):
                part = block[top : top + 8]
                column = jnp.take_along_axis(part, index, axis=1)
                block[top : top + 8] = jnp.where(other, 0.0, part) - column * row
        for node, block in enumerate(work):
            block[pl.ds(k, 1), :] = scaled[node : node + 1]
        return carry

    lax.fori_loop(0, B, step, 0)
    for node in range(nodes):
        out[node] = work[node][...]


def invert(ahead, behind, shift):
    nodes = shift.shape[0]
    return pl.pallas_call(
        invert_kernel,
        out_shape=jax.ShapeDtypeStruct((nodes, B, B), jnp.float32),
        in_specs=[VMEM] * 3,
        out_specs=VMEM,
        scratch_shapes=[pltpu.VMEM((B, B), jnp.float32)] * nodes,
    )(ahead, behind, shift)


def spring_kernel(factors, out):
    for node in range(factors.shape[2]):
        first, second, _ = split(gram(factors[0, 0, node]))
        out[0, 0, node, :, :B] = first
        out[0, 0, node, :, B:] = second


def springs_of(factors):
    devices, directions, nodes = factors.shape[:3]
    return pl.pallas_call(
        spring_kernel,
        grid=(devices, directions),
        out_shape=jax.ShapeDtypeStruct((devices, directions, nodes, B, 2 * B), jnp.bfloat16),
        in_specs=[pl.BlockSpec((1, 1, nodes, B, B), lambda i, d: (i, d, 0, 0, 0))],
        out_specs=pl.BlockSpec((1, 1, nodes, B, 2 * B), lambda i, d: (i, d, 0, 0, 0)),
    )(factors)


def stacked(value):
    first, second, third = (term.astype(jnp.float32) for term in split(value))
    upper = lax.broadcasted_iota(jnp.int32, value.shape, 0) < ROWS
    both = [jnp.where(upper, first, second), jnp.where(upper, third, 0.0)]
    return jnp.concatenate(both, axis=0).astype(jnp.bfloat16)


def product(left, right):
    full = jnp.dot(left, right, preferred_element_type=jnp.float32)
    total = full[: 2 * ROWS, :B] + full[2 * ROWS :, :B]
    for part in range(1, right.shape[1] // B):
        total = total + full[: 2 * ROWS, part * B : (part + 1) * B]
    return total + jnp.concatenate([total[ROWS:], total[:ROWS]], axis=0)


def solve_kernel(nx, ny, nbx, nby):
    ncy = ny // nby
    devices = (nx // nbx) * ncy
    unroll = 4 if ny % 4 == 0 else 1

    def kernel(load, shift, springs, inverse, out_x, out_r, w, m, p, q, image, x, r, z, mass, sem):
        pull = pltpu.make_async_copy(springs, w, sem)
        pull.start()

        def prepare(dev, carry):
            for lx in range(nbx):
                for ly in range(nby):
                    gx, gy = (dev // ncy) * nbx + lx, (dev % ncy) * nby + ly
                    node = lx * nby + ly
                    for part, term in enumerate(split(inverse[dev, node])):
                        m[gx, gy, :, part * B : (part + 1) * B] = term
                    field = load[dev, node]
                    r[gx, gy] = jnp.concatenate([field, field], axis=0)
                    mass[gx, gy] = jnp.broadcast_to(shift[dev, pl.ds(node, 1), :], (2 * ROWS, B))
            return carry

        lax.fori_loop(0, devices, prepare, 0)
        p[...] = jnp.zeros_like(p)
        q[...] = jnp.zeros_like(q)
        x[...] = jnp.zeros_like(x)
        zero = jnp.zeros((2 * ROWS, B), jnp.float32)

        def total(values):
            return jnp.sum(values, axis=1, keepdims=True)

        def iterate(_, rz_old):
            def precondition(y, acc):
                for i in range(nx):
                    value = r[i, y]
                    precon = product(stacked(value), m[i, y])
                    z[i, y] = precon
                    acc = acc + value * precon
                return acc

            rz = total(lax.fori_loop(0, ny, precondition, zero, unroll=unroll))
            ratio = rz / rz_old

            def advance(y, carry):
                for i in range(nx):
                    p[1 + i, 1 + y] = z[i, y] + ratio * p[1 + i, 1 + y]
                return carry

            lax.fori_loop(0, ny, advance, 0, unroll=unroll)

            def edges(dev, carry):
                for node in range(nbx * nby):
                    x_at = 1 + (dev // ncy) * nbx + node // nby
                    y_at = 1 + (dev % ncy) * nby + node % nby
                    for d, (step_x, step_y) in enumerate(OFFSETS):
                        delta = p[x_at, y_at] - p[x_at + step_x, y_at + step_y]
                        q[d, x_at, y_at] = product(stacked(delta), w[dev, d, node])
                return carry

            lax.fori_loop(0, devices, edges, 0)

            def gather(y, acc):
                for i in range(nx):
                    value = p[1 + i, 1 + y]
                    result = mass[i, y] * value
                    for d, (step_x, step_y) in enumerate(OFFSETS):
                        result = result + (
                            q[d, 1 + i, 1 + y] - q[d, 1 + i - step_x, 1 + y - step_y]
                        )
                    image[i, y] = result
                    acc = acc + value * result
                return acc

            alpha = rz / total(lax.fori_loop(0, ny, gather, zero, unroll=unroll))

            def update(y, carry):
                for i in range(nx):
                    x[i, y] = x[i, y] + alpha * p[1 + i, 1 + y]
                    r[i, y] = r[i, y] - alpha * image[i, y]
                return carry

            lax.fori_loop(0, ny, update, 0, unroll=unroll)
            return rz

        pull.wait()
        lax.fori_loop(0, ITERS, iterate, jnp.ones((2 * ROWS, 1), jnp.float32))

        def finish(dev, carry):
            for lx in range(nbx):
                for ly in range(nby):
                    gx, gy = (dev // ncy) * nbx + lx, (dev % ncy) * nby + ly
                    out_x[dev, lx * nby + ly] = x[gx, gy][:ROWS]
                    out_r[dev, lx * nby + ly] = r[gx, gy][:ROWS]
            return carry

        lax.fori_loop(0, devices, finish, 0)

    return kernel


def solve(load, shift, springs, inverse, nx, ny, nbx, nby):
    tall = 2 * ROWS
    field = pltpu.VMEM((nx, ny, tall, B), jnp.float32)
    return pl.pallas_call(
        solve_kernel(nx, ny, nbx, nby),
        out_shape=[jax.ShapeDtypeStruct(load.shape, jnp.float32)] * 2,
        in_specs=[VMEM, VMEM, pl.BlockSpec(memory_space=pl.ANY), VMEM],
        out_specs=[VMEM] * 2,
        scratch_shapes=[
            pltpu.VMEM(springs.shape, jnp.bfloat16),
            pltpu.VMEM((nx, ny, B, 3 * B), jnp.bfloat16),
            pltpu.VMEM((nx + 2, ny + 2, tall, B), jnp.float32),
            pltpu.VMEM((len(OFFSETS), nx + 2, ny + 2, tall, B), jnp.float32),
        ]
        + [field] * 5
        + [pltpu.SemaphoreType.DMA(())],
        compiler_params=pltpu.CompilerParams(vmem_limit_bytes=VMEM_BYTES),
    )(load, shift, springs, inverse)


def shifted(cells, axis, dim, step):
    count = lax.axis_size(axis)
    size = cells.shape[dim]
    if step == 1:
        rim = lax.slice_in_dim(cells, size - 1, size, axis=dim)
        rim = lax.ppermute(rim, axis, [(i, i + 1) for i in range(count - 1)])
        return jnp.concatenate([rim, lax.slice_in_dim(cells, 0, size - 1, axis=dim)], axis=dim)
    rim = lax.slice_in_dim(cells, 0, 1, axis=dim)
    rim = lax.ppermute(rim, axis, [(i + 1, i) for i in range(count - 1)])
    return jnp.concatenate([lax.slice_in_dim(cells, 1, size, axis=dim), rim], axis=dim)


def local_columns(load, factors, links, shift):
    nbx, nby, rhs, _ = load.shape
    gx, gy = (lax.axis_size(axis) for axis in GRID_AXES)
    devices, nodes = gx * gy, nbx * nby
    masked = factors * links.astype(jnp.bfloat16)[:, :, :, None, None]
    gathered = lax.all_gather(masked.reshape(4, nodes, B, B), GRID_AXES)
    down = shifted(jnp.stack([masked[0], masked[2], masked[3]]), "gx", 1, 1)
    left = shifted(jnp.stack([masked[1], down[1]]), "gy", 2, 1)
    right = shifted(down[2:], "gy", 2, -1)
    behind = jnp.stack([down[0], left[0], left[1], right[0]])
    flat_shift = shift.reshape(nodes, B)
    inverse = invert(
        masked.reshape(4, nodes, B, B), behind.reshape(4, nodes, B, B), flat_shift
    )
    columns = load.reshape(nodes, devices, ROWS, B).transpose(1, 0, 2, 3)
    columns = lax.all_to_all(columns, GRID_AXES, 0, 0)
    shifts = lax.all_gather(flat_shift, GRID_AXES)
    gathered, inverse = lax.optimization_barrier((gathered, inverse))
    inverses = lax.all_gather(inverse, GRID_AXES)
    springs = springs_of(gathered)
    outs = solve(columns, shifts, springs, inverses, gx * nbx, gy * nby, nbx, nby)
    outs = lax.all_to_all(jnp.stack(outs, axis=1), GRID_AXES, 0, 0)
    outs = outs.transpose(1, 2, 0, 3, 4).reshape(2, nbx, nby, rhs, B)
    return (outs[0], outs[1])


def local(load, factors, links, shift):
    devices = lax.axis_size("gx") * lax.axis_size("gy")
    blocks = devices * load.shape[0] * load.shape[1]
    held = blocks * B * B * (len(OFFSETS) * 6 + 10)
    if load.shape[2] == ROWS * devices and held < VMEM_BYTES * 3 // 4:
        return local_columns(load, factors, links, shift)
    return local_halo(load, factors, links, shift)


def solution(mesh):
    placed = (
        P(("case", "gx"), "gy", None, None),
        P(None, ("case", "gx"), "gy", None, None),
        P(None, ("case", "gx"), "gy"),
        P(("case", "gx"), "gy", None),
    )
    return jax.shard_map(
        local,
        mesh=mesh,
        in_specs=placed,
        out_specs=(P(("case", "gx"), "gy", None, None), P(("case", "gx"), "gy", None, None)),
        check_vma=False,
    )
```

```python
import jax
import jax.numpy as jnp
from jax import lax
from jax.experimental import pallas as pl
from jax.experimental.pallas import tpu as pltpu
from jax.sharding import PartitionSpec as P

B = 128
ITERS = 8


OFFSETS = ((1, 0), (0, 1), (1, 1), (1, -1))
PRECISE = lax.Precision.HIGHEST


def extended(cells, sides, width):
    for axis, dim in sides:
        count = lax.axis_size(axis)
        ends = count - 1
        head = lax.slice_in_dim(cells, 0, width, axis=dim)
        tail = lax.slice_in_dim(cells, cells.shape[dim] - width, cells.shape[dim], axis=dim)
        cells = jnp.concatenate(
            [
                lax.ppermute(tail, axis, [(i, (i + 1) % count) for i in range(ends)]),
                cells,
                lax.ppermute(head, axis, [((i + 1) % count, i) for i in range(ends)]),
            ],
            axis=dim,
        )
    return cells


def window(padded, step_x, step_y, count_x, count_y):
    return padded[1 + step_x : 1 + step_x + count_x, 1 + step_y : 1 + step_y + count_y]


def inner(left, right):
    return jnp.sum(left * right, axis=(0, 1, 3))


def spread(values):
    return values[None, None, :, None]


def local_halo(load, factors, links, shift):
    count_x, count_y = (load.shape[0], load.shape[1])
    masked = factors * links.astype(jnp.bfloat16)[:, :, :, None, None]
    springs = (
        jnp.einsum("dxyak,dxybk->dxyab", masked, masked, preferred_element_type=jnp.float32) / B
    )
    padded_springs = extended(springs, (("gx", 1), ("gy", 2)), 1)
    forward = padded_springs[:, 1:-1, 1:-1]
    backward = jnp.stack(
        [
            window(
                padded_springs[offset], -OFFSETS[offset][0], -OFFSETS[offset][1], count_x, count_y
            )
            for offset in range(4)
        ]
    )
    identity = jnp.eye(B, dtype=jnp.float32)
    diagonal = shift[..., None] * identity + jnp.sum(forward, axis=0) + jnp.sum(backward, axis=0)
    lower = jnp.linalg.cholesky(diagonal.reshape(-1, B, B))
    inverse = jax.vmap(lambda factor: jax.scipy.linalg.cho_solve((factor, True), identity))(
        lower
    ).reshape(diagonal.shape)
    blocks = jnp.concatenate([diagonal[None], -forward, -backward], axis=0)

    def operate(field):
        padded = extended(field, (("gx", 0), ("gy", 1)), 1)
        pieces = [field]
        pieces = pieces + [
            window(padded, step_x, step_y, count_x, count_y) for step_x, step_y in OFFSETS
        ]
        pieces = pieces + [
            window(padded, -step_x, -step_y, count_x, count_y) for step_x, step_y in OFFSETS
        ]
        return jnp.einsum(
            "kxyab,kxyrb->xyra",
            blocks,
            jnp.stack(pieces),
            precision=PRECISE,
            preferred_element_type=jnp.float32,
        )

    def precondition(field):
        return jnp.einsum(
            "xyab,xyrb->xyra", inverse, field, precision=PRECISE, preferred_element_type=jnp.float32
        )

    def paired(residual, precon, image):
        return lax.psum((inner(residual, precon), inner(image, precon)), ("gx", "gy"))

    solution = jnp.zeros_like(load)
    residual = load
    precon = precondition(residual)
    image = operate(precon)
    gamma, delta = paired(residual, precon, image)
    alpha = gamma / delta
    direction, along = (precon, image)
    for iteration in range(ITERS):
        solution = solution + spread(alpha) * direction
        residual = residual - spread(alpha) * along
        if iteration + 1 < ITERS:
            precon = precondition(residual)
            image = operate(precon)
            gamma_next, delta = paired(residual, precon, image)
            ratio = gamma_next / gamma
            alpha = gamma_next / (delta - ratio * gamma_next / alpha)
            direction = precon + spread(ratio) * direction
            along = image + spread(ratio) * along
            gamma = gamma_next
    return (solution, residual)


GRID_AXES = ("gx", "gy")
ROWS = 4
VMEM = pl.BlockSpec(memory_space=pltpu.VMEM)
VMEM_BYTES = 56 * 1024 * 1024


def gram(block):
    return (
        lax.dot_general(block, block, (((1,), (1,)), ((), ())), preferred_element_type=jnp.float32)
        / B
    )


def split(value):
    first = value.astype(jnp.bfloat16)
    rest = value - first.astype(jnp.float32)
    second = rest.astype(jnp.bfloat16)
    third = (rest - second.astype(jnp.float32)).astype(jnp.bfloat16)
    return first, second, third


def invert_kernel(ahead, behind, shift, out, *work):
    nodes = shift.shape[0]
    rows = lax.broadcasted_iota(jnp.int32, (B, B), 0)
    lanes = lax.broadcasted_iota(jnp.int32, (B, B), 1)
    for node in range(nodes):
        total = jnp.where(rows == lanes, shift[pl.ds(node, 1), :], 0.0)
        for d in range(len(OFFSETS)):
            total = total + gram(ahead[d, node])
            total = total + gram(behind[d, node])
        work[node][...] = total

    def step(k, carry):
        lane = lax.broadcasted_iota(jnp.int32, (nodes, B), 1)
        picked = jnp.concatenate([block[pl.ds(k, 1), :] for block in work], axis=0)
        pivot = jnp.sum(jnp.where(lane == k, picked, 0.0), axis=1, keepdims=True)
        scaled = jnp.where(lane == k, 1.0, picked) / pivot
        index = jnp.full((8, B), k, jnp.int32)
        other = lane[:1] == k
        for node, block in enumerate(work):
            row = scaled[node : node + 1]
            for top in range(0, B, 8):
                part = block[top : top + 8]
                column = jnp.take_along_axis(part, index, axis=1)
                block[top : top + 8] = jnp.where(other, 0.0, part) - column * row
        for node, block in enumerate(work):
            block[pl.ds(k, 1), :] = scaled[node : node + 1]
        return carry

    lax.fori_loop(0, B, step, 0)
    pairs = (nodes + 1) // 2
    out[pairs * B :] = jnp.zeros((out.shape[0] - pairs * B, B), jnp.float32)
    for pair in range(pairs):
        lower = work[2 * pair][...]
        upper = work[min(2 * pair + 1, nodes - 1)][...]
        lower = 0.5 * (lower + lower.T)
        upper = 0.5 * (upper + upper.T)
        out[pair * B : (pair + 1) * B] = jnp.where(rows >= lanes, lower, upper)
        diagonal = jnp.sum(jnp.where(rows == lanes, upper, 0.0), axis=0, keepdims=True)
        out[pairs * B + pair : pairs * B + pair + 1] = diagonal


def unpacked(packed, diagonal):
    rows = lax.broadcasted_iota(jnp.int32, (B, B), 0)
    lanes = lax.broadcasted_iota(jnp.int32, (B, B), 1)
    turned = packed.T
    lower = jnp.where(rows >= lanes, packed, turned)
    upper = jnp.where(rows < lanes, packed, turned)
    return lower, jnp.where(rows == lanes, diagonal, upper)


def invert(ahead, behind, shift):
    nodes = shift.shape[0]
    pairs = (nodes + 1) // 2
    return pl.pallas_call(
        invert_kernel,
        out_shape=jax.ShapeDtypeStruct((pairs * B + (pairs + 7) // 8 * 8, B), jnp.float32),
        in_specs=[VMEM] * 3,
        out_specs=VMEM,
        scratch_shapes=[pltpu.VMEM((B, B), jnp.float32)] * nodes,
    )(ahead, behind, shift)


def spring_kernel(factors, small, out):
    _, directions, nodes = factors.shape[:3]
    for node in range(nodes):
        for d in range(directions):
            link = small[0, node : node + 1, B + d : B + d + 1]
            first, second, _ = split(gram(factors[0, d, node]) * link)
            out[0, d, node, :, :B] = first
            out[0, d, node, :, B:] = second


def springs_of(factors, small):
    devices, directions, nodes = factors.shape[:3]
    return pl.pallas_call(
        spring_kernel,
        grid=(devices,),
        out_shape=jax.ShapeDtypeStruct((devices, directions, nodes, B, 2 * B), jnp.bfloat16),
        in_specs=[
            pl.BlockSpec((1, directions, nodes, B, B), lambda i: (i, 0, 0, 0, 0)),
            pl.BlockSpec((1, nodes, 2 * B), lambda i: (i, 0, 0)),
        ],
        out_specs=pl.BlockSpec((1, directions, nodes, B, 2 * B), lambda i: (i, 0, 0, 0, 0)),
    )(factors, small)


def stacked(value):
    first, second, third = (term.astype(jnp.float32) for term in split(value))
    upper = lax.broadcasted_iota(jnp.int32, value.shape, 0) < ROWS
    both = [jnp.where(upper, first, second), jnp.where(upper, third, 0.0)]
    return jnp.concatenate(both, axis=0).astype(jnp.bfloat16)


def product(left, right):
    full = jnp.dot(left, right, preferred_element_type=jnp.float32)
    total = full[: 2 * ROWS, :B] + full[2 * ROWS :, :B]
    for part in range(1, right.shape[1] // B):
        total = total + full[: 2 * ROWS, part * B : (part + 1) * B]
    return total + jnp.concatenate([total[ROWS:], total[:ROWS]], axis=0)


def solve_kernel(nx, ny, nbx, nby):
    ncy = ny // nby
    devices = (nx // nbx) * ncy
    pairs = (nbx * nby + 1) // 2
    unroll = next(step for step in (8, 6, 4, 3, 2, 1) if ny % step == 0)

    def kernel(load, small, springs, inverse, out, w, m, p, q, image, x, r, z, mass, sem):
        pull = pltpu.make_async_copy(springs, w, sem)
        pull.start()

        def prepare(dev, carry):
            for lx in range(nbx):
                for ly in range(nby):
                    gx, gy = (dev // ncy) * nbx + lx, (dev % ncy) * nby + ly
                    node = lx * nby + ly
                    if node % 2 == 0:
                        at = pairs * B + node // 2
                        blocks = unpacked(
                            inverse[dev, node // 2 * B : (node // 2 + 1) * B],
                            inverse[dev, at : at + 1],
                        )
                    for part, term in enumerate(split(blocks[node % 2])):
                        m[gx, gy, :, part * B : (part + 1) * B] = term
                    field = load[dev, node]
                    r[gx, gy] = jnp.concatenate([field, field], axis=0)
                    mass[gx, gy] = jnp.broadcast_to(small[dev, node : node + 1, :B], (2 * ROWS, B))
            return carry

        lax.fori_loop(0, devices, prepare, 0)
        p[...] = jnp.zeros_like(p)
        q[...] = jnp.zeros_like(q)
        x[...] = jnp.zeros_like(x)
        image[...] = jnp.zeros_like(image)
        zero = jnp.zeros((2 * ROWS, B), jnp.float32)

        def total(values):
            return jnp.sum(values, axis=1, keepdims=True)

        def iterate(_, carried):
            rz_old, alpha = carried

            def precondition(y, acc):
                for i in range(nx):
                    value = r[i, y] - alpha * image[i, y]
                    r[i, y] = value
                    x[i, y] = x[i, y] + alpha * p[1 + i, 1 + y]
                    precon = product(stacked(value), m[i, y])
                    z[i, y] = precon
                    acc = acc + value * precon
                return acc

            rz = total(lax.fori_loop(0, ny, precondition, zero, unroll=unroll))
            ratio = rz / rz_old

            def advance(y, carry):
                for i in range(nx):
                    p[1 + i, 1 + y] = z[i, y] + ratio * p[1 + i, 1 + y]
                return carry

            lax.fori_loop(0, ny, advance, 0, unroll=unroll)

            def edges(dev, carry):
                for node in range(nbx * nby):
                    x_at = 1 + (dev // ncy) * nbx + node // nby
                    y_at = 1 + (dev % ncy) * nby + node % nby
                    for d, (step_x, step_y) in enumerate(OFFSETS):
                        delta = p[x_at, y_at] - p[x_at + step_x, y_at + step_y]
                        q[d, x_at, y_at] = product(stacked(delta), w[dev, d, node])
                return carry

            lax.fori_loop(0, devices, edges, 0)

            def gather(y, acc):
                for i in range(nx):
                    value = p[1 + i, 1 + y]
                    result = mass[i, y] * value
                    for d, (step_x, step_y) in enumerate(OFFSETS):
                        result = result + (
                            q[d, 1 + i, 1 + y] - q[d, 1 + i - step_x, 1 + y - step_y]
                        )
                    image[i, y] = result
                    acc = acc + value * result
                return acc

            alpha = rz / total(lax.fori_loop(0, ny, gather, zero, unroll=unroll))

            return rz, alpha

        pull.wait()
        one = jnp.ones((2 * ROWS, 1), jnp.float32)
        _, alpha = lax.fori_loop(0, ITERS, iterate, (one, jnp.zeros_like(one)))

        def finish(dev, carry):
            for lx in range(nbx):
                for ly in range(nby):
                    gx, gy = (dev // ncy) * nbx + lx, (dev % ncy) * nby + ly
                    out[dev, 0, lx * nby + ly] = (x[gx, gy] + alpha * p[1 + gx, 1 + gy])[:ROWS]
                    out[dev, 1, lx * nby + ly] = (r[gx, gy] - alpha * image[gx, gy])[:ROWS]
            return carry

        lax.fori_loop(0, devices, finish, 0)

    return kernel


def solve(load, small, springs, inverse, nx, ny, nbx, nby):
    tall = 2 * ROWS
    field = pltpu.VMEM((nx, ny, tall, B), jnp.float32)
    return pl.pallas_call(
        solve_kernel(nx, ny, nbx, nby),
        out_shape=jax.ShapeDtypeStruct((load.shape[0], 2) + load.shape[1:], jnp.float32),
        in_specs=[VMEM, VMEM, pl.BlockSpec(memory_space=pl.ANY), VMEM],
        out_specs=VMEM,
        scratch_shapes=[
            pltpu.VMEM(springs.shape, jnp.bfloat16),
            pltpu.VMEM((nx, ny, B, 3 * B), jnp.bfloat16),
            pltpu.VMEM((nx + 2, ny + 2, tall, B), jnp.float32),
            pltpu.VMEM((len(OFFSETS), nx + 2, ny + 2, tall, B), jnp.float32),
        ]
        + [field] * 5
        + [pltpu.SemaphoreType.DMA(())],
        compiler_params=pltpu.CompilerParams(vmem_limit_bytes=VMEM_BYTES),
    )(load, small, springs, inverse)


def shifted(cells, axis, dim, step):
    count = lax.axis_size(axis)
    size = cells.shape[dim]
    if step == 1:
        rim = lax.slice_in_dim(cells, size - 1, size, axis=dim)
        rim = lax.ppermute(rim, axis, [(i, i + 1) for i in range(count - 1)])
        return jnp.concatenate([rim, lax.slice_in_dim(cells, 0, size - 1, axis=dim)], axis=dim)
    rim = lax.slice_in_dim(cells, 0, 1, axis=dim)
    rim = lax.ppermute(rim, axis, [(i + 1, i) for i in range(count - 1)])
    return jnp.concatenate([lax.slice_in_dim(cells, 1, size, axis=dim), rim], axis=dim)


def local_columns(load, factors, links, shift):
    nbx, nby, rhs, _ = load.shape
    gx, gy = (lax.axis_size(axis) for axis in GRID_AXES)
    devices, nodes = gx * gy, nbx * nby
    gathered = lax.all_gather(factors.reshape(4, nodes, B, B), GRID_AXES)
    masked = factors * links.astype(jnp.bfloat16)[:, :, :, None, None]
    down = shifted(jnp.stack([masked[0], masked[2], masked[3]]), "gx", 1, 1)
    flat_links = links.reshape(len(OFFSETS), nodes).T.astype(jnp.float32)
    flat_links = jnp.pad(flat_links, ((0, 0), (0, B - len(OFFSETS))))
    small = jnp.concatenate([shift.reshape(nodes, B), flat_links], axis=1)
    small = lax.all_gather(small, GRID_AXES)
    columns = load.reshape(nodes, devices, ROWS, B).transpose(1, 0, 2, 3)
    columns = lax.all_to_all(columns, GRID_AXES, 0, 0)
    down, small, columns = lax.optimization_barrier((down, small, columns))
    left = shifted(jnp.stack([masked[1], down[1]]), "gy", 2, 1)
    right = shifted(down[2:], "gy", 2, -1)
    behind = jnp.stack([down[0], left[0], left[1], right[0]])
    inverse = invert(
        masked.reshape(4, nodes, B, B), behind.reshape(4, nodes, B, B), shift.reshape(nodes, B)
    )
    gathered, inverse = lax.optimization_barrier((gathered, inverse))
    inverses = lax.all_gather(inverse, GRID_AXES)
    springs = springs_of(gathered, small)
    outs = solve(columns, small, springs, inverses, gx * nbx, gy * nby, nbx, nby)
    outs = lax.all_to_all(outs, GRID_AXES, 0, 0)
    outs = outs.transpose(1, 2, 0, 3, 4).reshape(2, nbx, nby, rhs, B)
    return (outs[0], outs[1])


def local(load, factors, links, shift):
    devices = lax.axis_size("gx") * lax.axis_size("gy")
    blocks = devices * load.shape[0] * load.shape[1]
    held = blocks * B * B * (len(OFFSETS) * 6 + 10)
    if load.shape[2] == ROWS * devices and held < VMEM_BYTES * 3 // 4:
        return local_columns(load, factors, links, shift)
    return local_halo(load, factors, links, shift)


def solution(mesh):
    placed = (
        P(("case", "gx"), "gy", None, None),
        P(None, ("case", "gx"), "gy", None, None),
        P(None, ("case", "gx"), "gy"),
        P(("case", "gx"), "gy", None),
    )
    return jax.shard_map(
        local,
        mesh=mesh,
        in_specs=placed,
        out_specs=(P(("case", "gx"), "gy", None, None), P(("case", "gx"), "gy", None, None)),
        check_vma=False,
    )
```

```python
import jax
import jax.numpy as jnp
from jax import lax
from jax.experimental import pallas as pl
from jax.experimental.pallas import tpu as pltpu
from jax.sharding import PartitionSpec as P

B = 128
ITERS = 8


OFFSETS = ((1, 0), (0, 1), (1, 1), (1, -1))
PRECISE = lax.Precision.HIGHEST


def extended(cells, sides, width):
    for axis, dim in sides:
        count = lax.axis_size(axis)
        ends = count - 1
        head = lax.slice_in_dim(cells, 0, width, axis=dim)
        tail = lax.slice_in_dim(cells, cells.shape[dim] - width, cells.shape[dim], axis=dim)
        cells = jnp.concatenate(
            [
                lax.ppermute(tail, axis, [(i, (i + 1) % count) for i in range(ends)]),
                cells,
                lax.ppermute(head, axis, [((i + 1) % count, i) for i in range(ends)]),
            ],
            axis=dim,
        )
    return cells


def window(padded, step_x, step_y, count_x, count_y):
    return padded[1 + step_x : 1 + step_x + count_x, 1 + step_y : 1 + step_y + count_y]


def inner(left, right):
    return jnp.sum(left * right, axis=(0, 1, 3))


def spread(values):
    return values[None, None, :, None]


def local_halo(load, factors, links, shift):
    count_x, count_y = (load.shape[0], load.shape[1])
    masked = factors * links.astype(jnp.bfloat16)[:, :, :, None, None]
    springs = (
        jnp.einsum("dxyak,dxybk->dxyab", masked, masked, preferred_element_type=jnp.float32) / B
    )
    padded_springs = extended(springs, (("gx", 1), ("gy", 2)), 1)
    forward = padded_springs[:, 1:-1, 1:-1]
    backward = jnp.stack(
        [
            window(
                padded_springs[offset], -OFFSETS[offset][0], -OFFSETS[offset][1], count_x, count_y
            )
            for offset in range(4)
        ]
    )
    identity = jnp.eye(B, dtype=jnp.float32)
    diagonal = shift[..., None] * identity + jnp.sum(forward, axis=0) + jnp.sum(backward, axis=0)
    lower = jnp.linalg.cholesky(diagonal.reshape(-1, B, B))
    inverse = jax.vmap(lambda factor: jax.scipy.linalg.cho_solve((factor, True), identity))(
        lower
    ).reshape(diagonal.shape)
    blocks = jnp.concatenate([diagonal[None], -forward, -backward], axis=0)

    def operate(field):
        padded = extended(field, (("gx", 0), ("gy", 1)), 1)
        pieces = [field]
        pieces = pieces + [
            window(padded, step_x, step_y, count_x, count_y) for step_x, step_y in OFFSETS
        ]
        pieces = pieces + [
            window(padded, -step_x, -step_y, count_x, count_y) for step_x, step_y in OFFSETS
        ]
        return jnp.einsum(
            "kxyab,kxyrb->xyra",
            blocks,
            jnp.stack(pieces),
            precision=PRECISE,
            preferred_element_type=jnp.float32,
        )

    def precondition(field):
        return jnp.einsum(
            "xyab,xyrb->xyra", inverse, field, precision=PRECISE, preferred_element_type=jnp.float32
        )

    def paired(residual, precon, image):
        return lax.psum((inner(residual, precon), inner(image, precon)), ("gx", "gy"))

    solution = jnp.zeros_like(load)
    residual = load
    precon = precondition(residual)
    image = operate(precon)
    gamma, delta = paired(residual, precon, image)
    alpha = gamma / delta
    direction, along = (precon, image)
    for iteration in range(ITERS):
        solution = solution + spread(alpha) * direction
        residual = residual - spread(alpha) * along
        if iteration + 1 < ITERS:
            precon = precondition(residual)
            image = operate(precon)
            gamma_next, delta = paired(residual, precon, image)
            ratio = gamma_next / gamma
            alpha = gamma_next / (delta - ratio * gamma_next / alpha)
            direction = precon + spread(ratio) * direction
            along = image + spread(ratio) * along
            gamma = gamma_next
    return (solution, residual)


GRID_AXES = ("gx", "gy")
ROWS = 4
VMEM = pl.BlockSpec(memory_space=pltpu.VMEM)
VMEM_BYTES = 56 * 1024 * 1024


def gram(block):
    return (
        lax.dot_general(block, block, (((1,), (1,)), ((), ())), preferred_element_type=jnp.float32)
        / B
    )


def split(value):
    first = value.astype(jnp.bfloat16)
    rest = value - first.astype(jnp.float32)
    second = rest.astype(jnp.bfloat16)
    third = (rest - second.astype(jnp.float32)).astype(jnp.bfloat16)
    return first, second, third


def invert_kernel(ahead, behind, shift, out, *work):
    nodes = shift.shape[0]
    rows = lax.broadcasted_iota(jnp.int32, (B, B), 0)
    lanes = lax.broadcasted_iota(jnp.int32, (B, B), 1)
    for node in range(nodes):
        total = jnp.where(rows == lanes, shift[pl.ds(node, 1), :], 0.0)
        for d in range(len(OFFSETS)):
            total = total + gram(ahead[d, node])
            total = total + gram(behind[d, node])
        work[node][...] = total

    lane = lax.broadcasted_iota(jnp.int32, (nodes, B), 1)

    def picked(k):
        return jnp.concatenate([block[pl.ds(k, 1), :] for block in work], axis=0)

    def entry(values, k):
        return jnp.sum(jnp.where(lane == k, values, 0.0), axis=1, keepdims=True)

    def step(k, scaled):
        coming = picked(jnp.minimum(k + 1, B - 1))
        factor = entry(coming, k)
        pivot = entry(coming, k + 1) - factor * entry(scaled, k + 1)
        coming = jnp.where(lane == k, 0.0, coming) - factor * scaled
        following = jnp.where(lane == k + 1, 1.0, coming) / pivot
        index = jnp.full((8, B), k, jnp.int32)
        other = lane[:1] == k
        for node, block in enumerate(work):
            row = scaled[node : node + 1]
            for top in range(0, B, 8):
                part = block[top : top + 8]
                column = jnp.take_along_axis(part, index, axis=1)
                block[top : top + 8] = jnp.where(other, 0.0, part) - column * row
        for node, block in enumerate(work):
            block[pl.ds(k, 1), :] = scaled[node : node + 1]
        return following

    first = picked(0)
    lax.fori_loop(0, B, step, jnp.where(lane == 0, 1.0, first) / entry(first, 0))
    pairs = (nodes + 1) // 2
    out[pairs * B :] = jnp.zeros((out.shape[0] - pairs * B, B), jnp.float32)
    for pair in range(pairs):
        lower = work[2 * pair][...]
        upper = work[min(2 * pair + 1, nodes - 1)][...]
        lower = 0.5 * (lower + lower.T)
        upper = 0.5 * (upper + upper.T)
        out[pair * B : (pair + 1) * B] = jnp.where(rows >= lanes, lower, upper)
        diagonal = jnp.sum(jnp.where(rows == lanes, upper, 0.0), axis=0, keepdims=True)
        out[pairs * B + pair : pairs * B + pair + 1] = diagonal


def unpacked(packed, diagonal):
    rows = lax.broadcasted_iota(jnp.int32, (B, B), 0)
    lanes = lax.broadcasted_iota(jnp.int32, (B, B), 1)
    turned = packed.T
    lower = jnp.where(rows >= lanes, packed, turned)
    upper = jnp.where(rows < lanes, packed, turned)
    return lower, jnp.where(rows == lanes, diagonal, upper)


def invert(ahead, behind, shift):
    nodes = shift.shape[0]
    pairs = (nodes + 1) // 2
    return pl.pallas_call(
        invert_kernel,
        out_shape=jax.ShapeDtypeStruct((pairs * B + (pairs + 7) // 8 * 8, B), jnp.float32),
        in_specs=[VMEM] * 3,
        out_specs=VMEM,
        scratch_shapes=[pltpu.VMEM((B, B), jnp.float32)] * nodes,
    )(ahead, behind, shift)


def spring_kernel(factors, small, out):
    _, directions, nodes = factors.shape[:3]
    for node in range(nodes):
        for d in range(directions):
            link = small[0, node : node + 1, B + d : B + d + 1]
            first, second, _ = split(gram(factors[0, d, node]) * link)
            out[0, d, node, :, :B] = first
            out[0, d, node, :, B:] = second


def springs_of(factors, small):
    devices, directions, nodes = factors.shape[:3]
    return pl.pallas_call(
        spring_kernel,
        grid=(devices,),
        out_shape=jax.ShapeDtypeStruct((devices, directions, nodes, B, 2 * B), jnp.bfloat16),
        in_specs=[
            pl.BlockSpec((1, directions, nodes, B, B), lambda i: (i, 0, 0, 0, 0)),
            pl.BlockSpec((1, nodes, 2 * B), lambda i: (i, 0, 0)),
        ],
        out_specs=pl.BlockSpec((1, directions, nodes, B, 2 * B), lambda i: (i, 0, 0, 0, 0)),
    )(factors, small)


def stacked(value):
    first, second, third = (term.astype(jnp.float32) for term in split(value))
    upper = lax.broadcasted_iota(jnp.int32, value.shape, 0) < ROWS
    both = [jnp.where(upper, first, second), jnp.where(upper, third, 0.0)]
    return jnp.concatenate(both, axis=0).astype(jnp.bfloat16)


def product(left, right):
    full = jnp.dot(left, right, preferred_element_type=jnp.float32)
    total = full[: 2 * ROWS, :B] + full[2 * ROWS :, :B]
    for part in range(1, right.shape[1] // B):
        total = total + full[: 2 * ROWS, part * B : (part + 1) * B]
    return total + jnp.concatenate([total[ROWS:], total[:ROWS]], axis=0)


def solve_kernel(nx, ny, nbx, nby):
    ncy = ny // nby
    devices = (nx // nbx) * ncy
    pairs = (nbx * nby + 1) // 2
    wide = ny // 2 if ny % 2 == 0 else 1
    unroll = next(step for step in (8, 6, 4, 3, 2, 1) if ny % step == 0)

    def kernel(load, small, springs, inverse, out, w, m, p, q, image, x, r, z, mass, sem):
        pull = pltpu.make_async_copy(springs, w, sem)
        pull.start()

        def prepare(dev, carry):
            for lx in range(nbx):
                for ly in range(nby):
                    gx, gy = (dev // ncy) * nbx + lx, (dev % ncy) * nby + ly
                    node = lx * nby + ly
                    if node % 2 == 0:
                        at = pairs * B + node // 2
                        blocks = unpacked(
                            inverse[dev, node // 2 * B : (node // 2 + 1) * B],
                            inverse[dev, at : at + 1],
                        )
                    for part, term in enumerate(split(blocks[node % 2])):
                        m[gx, gy, :, part * B : (part + 1) * B] = term
                    field = load[dev, node]
                    r[gx, gy] = jnp.concatenate([field, field], axis=0)
                    mass[gx, gy] = jnp.broadcast_to(small[dev, node : node + 1, :B], (2 * ROWS, B))
            return carry

        lax.fori_loop(0, devices, prepare, 0)
        p[...] = jnp.zeros_like(p)
        q[...] = jnp.zeros_like(q)
        x[...] = jnp.zeros_like(x)
        image[...] = jnp.zeros_like(image)
        zero = jnp.zeros((2 * ROWS, B), jnp.float32)

        def total(values):
            return jnp.sum(values, axis=1, keepdims=True)

        def iterate(_, carried):
            rz_old, alpha = carried

            def precondition(y, acc):
                for i in range(nx):
                    value = r[i, y] - alpha * image[i, y]
                    r[i, y] = value
                    x[i, y] = x[i, y] + alpha * p[1 + i, 1 + y]
                    precon = product(stacked(value), m[i, y])
                    z[i, y] = precon
                    acc = acc + value * precon
                return acc

            rz = total(lax.fori_loop(0, ny, precondition, zero, unroll=wide))
            ratio = rz / rz_old

            def advance(y, carry):
                for i in range(nx):
                    p[1 + i, 1 + y] = z[i, y] + ratio * p[1 + i, 1 + y]
                return carry

            lax.fori_loop(0, ny, advance, 0, unroll=unroll)

            def edges(dev, carry):
                for node in range(nbx * nby):
                    x_at = 1 + (dev // ncy) * nbx + node // nby
                    y_at = 1 + (dev % ncy) * nby + node % nby
                    for d, (step_x, step_y) in enumerate(OFFSETS):
                        delta = p[x_at, y_at] - p[x_at + step_x, y_at + step_y]
                        q[d, x_at, y_at] = product(stacked(delta), w[dev, d, node])
                return carry

            lax.fori_loop(0, devices, edges, 0, unroll=2 if devices % 2 == 0 else 1)

            def gather(y, acc):
                for i in range(nx):
                    value = p[1 + i, 1 + y]
                    result = mass[i, y] * value
                    for d, (step_x, step_y) in enumerate(OFFSETS):
                        result = result + (
                            q[d, 1 + i, 1 + y] - q[d, 1 + i - step_x, 1 + y - step_y]
                        )
                    image[i, y] = result
                    acc = acc + value * result
                return acc

            alpha = rz / total(lax.fori_loop(0, ny, gather, zero, unroll=unroll))

            return rz, alpha

        pull.wait()
        one = jnp.ones((2 * ROWS, 1), jnp.float32)
        _, alpha = lax.fori_loop(0, ITERS, iterate, (one, jnp.zeros_like(one)))

        def finish(dev, carry):
            for lx in range(nbx):
                for ly in range(nby):
                    gx, gy = (dev // ncy) * nbx + lx, (dev % ncy) * nby + ly
                    out[dev, 0, lx * nby + ly] = (x[gx, gy] + alpha * p[1 + gx, 1 + gy])[:ROWS]
                    out[dev, 1, lx * nby + ly] = (r[gx, gy] - alpha * image[gx, gy])[:ROWS]
            return carry

        lax.fori_loop(0, devices, finish, 0)

    return kernel


def solve(load, small, springs, inverse, nx, ny, nbx, nby):
    tall = 2 * ROWS
    field = pltpu.VMEM((nx, ny, tall, B), jnp.float32)
    return pl.pallas_call(
        solve_kernel(nx, ny, nbx, nby),
        out_shape=jax.ShapeDtypeStruct((load.shape[0], 2) + load.shape[1:], jnp.float32),
        in_specs=[VMEM, VMEM, pl.BlockSpec(memory_space=pl.ANY), VMEM],
        out_specs=VMEM,
        scratch_shapes=[
            pltpu.VMEM(springs.shape, jnp.bfloat16),
            pltpu.VMEM((nx, ny, B, 3 * B), jnp.bfloat16),
            pltpu.VMEM((nx + 2, ny + 2, tall, B), jnp.float32),
            pltpu.VMEM((len(OFFSETS), nx + 2, ny + 2, tall, B), jnp.float32),
        ]
        + [field] * 5
        + [pltpu.SemaphoreType.DMA(())],
        compiler_params=pltpu.CompilerParams(vmem_limit_bytes=VMEM_BYTES),
    )(load, small, springs, inverse)


def shifted(cells, axis, dim, step):
    count = lax.axis_size(axis)
    size = cells.shape[dim]
    if step == 1:
        rim = lax.slice_in_dim(cells, size - 1, size, axis=dim)
        rim = lax.ppermute(rim, axis, [(i, i + 1) for i in range(count - 1)])
        return jnp.concatenate([rim, lax.slice_in_dim(cells, 0, size - 1, axis=dim)], axis=dim)
    rim = lax.slice_in_dim(cells, 0, 1, axis=dim)
    rim = lax.ppermute(rim, axis, [(i + 1, i) for i in range(count - 1)])
    return jnp.concatenate([lax.slice_in_dim(cells, 1, size, axis=dim), rim], axis=dim)


def local_columns(load, factors, links, shift):
    nbx, nby, rhs, _ = load.shape
    gx, gy = (lax.axis_size(axis) for axis in GRID_AXES)
    devices, nodes = gx * gy, nbx * nby
    gathered = lax.all_gather(factors.reshape(4, nodes, B, B), GRID_AXES)
    masked = factors * links.astype(jnp.bfloat16)[:, :, :, None, None]
    down = shifted(jnp.stack([masked[0], masked[2], masked[3]]), "gx", 1, 1)
    flat_links = links.reshape(len(OFFSETS), nodes).T.astype(jnp.float32)
    flat_links = jnp.pad(flat_links, ((0, 0), (0, B - len(OFFSETS))))
    small = jnp.concatenate([shift.reshape(nodes, B), flat_links], axis=1)
    columns = load.reshape(nodes, devices, ROWS, B).transpose(1, 0, 2, 3)
    left = shifted(jnp.stack([masked[1], down[1]]), "gy", 2, 1)
    right = shifted(down[2:], "gy", 2, -1)
    behind = jnp.stack([down[0], left[0], left[1], right[0]])
    inverse = invert(
        masked.reshape(4, nodes, B, B), behind.reshape(4, nodes, B, B), shift.reshape(nodes, B)
    )
    gathered, inverse, small, columns = lax.optimization_barrier(
        (gathered, inverse, small, columns)
    )
    inverses = lax.all_gather(inverse, GRID_AXES)
    columns = lax.all_to_all(columns, GRID_AXES, 0, 0)
    small = lax.all_gather(small, GRID_AXES)
    springs = springs_of(gathered, small)
    outs = solve(columns, small, springs, inverses, gx * nbx, gy * nby, nbx, nby)
    outs = lax.all_to_all(outs, GRID_AXES, 0, 0)
    outs = outs.transpose(1, 2, 0, 3, 4).reshape(2, nbx, nby, rhs, B)
    return (outs[0], outs[1])


def local(load, factors, links, shift):
    devices = lax.axis_size("gx") * lax.axis_size("gy")
    blocks = devices * load.shape[0] * load.shape[1]
    held = blocks * B * B * (len(OFFSETS) * 6 + 10)
    if load.shape[2] == ROWS * devices and held < VMEM_BYTES * 3 // 4:
        return local_columns(load, factors, links, shift)
    return local_halo(load, factors, links, shift)


def solution(mesh):
    placed = (
        P(("case", "gx"), "gy", None, None),
        P(None, ("case", "gx"), "gy", None, None),
        P(None, ("case", "gx"), "gy"),
        P(("case", "gx"), "gy", None),
    )
    return jax.shard_map(
        local,
        mesh=mesh,
        in_specs=placed,
        out_specs=(P(("case", "gx"), "gy", None, None), P(("case", "gx"), "gy", None, None)),
        check_vma=False,
    )
```
